8 devices in a mesh: dp: 1 (over z), tp: 8 (over y, x, core).
Axes of the slice: x: 2, y: 2, z: 1, core: 2. Of those that a mesh axis runs over, the one named last changes fastest.
Arguments:
- hidden: bfloat16 [768, 1536], P('dp')
- tokens: int32 [768], P('dp')
- embedding: bfloat16 [151936, 1536], P('tp')
- head_w: bfloat16 [1536, 151936], P(None, 'tp')
- h_norm: float32 [1536], replicated
- e_norm: float32 [1536], replicated
- f_norm: float32 [1536], replicated
- o_norm: float32 [1536], replicated
- proj_w: bfloat16 [3072, 1536], P(None, 'tp')
- w_gate: bfloat16 [1536, 8960], P(None, 'tp')
- w_up: bfloat16 [1536, 8960], P(None, 'tp')
- w_down: bfloat16 [8960, 1536], P('tp')
Outputs:
- output 1: bfloat16 [768, 1536], P('dp')
- output 2: float32 [768, 151936], P('dp', 'tp')
All inputs are finite; a program needn't handle non-finite values.
Results may differ from the reference program's by a relative error of at most 0.0111966.
Values are sent between devices in bfloat16 or wider.
A program may use at most 1 GiB of HBM per device.

```python
import jax
import jax.numpy as jnp
from jax import lax

MODEL_DIM = 1536
VOCAB_SIZE = 151936
FFN_DIM = 8960
BATCH_ROWS = 768

HOT_WIDTH = VOCAB_SIZE // 32
NORM_EPS = 1e-6


def draw_tokens(key_in):
    sub_keys = jax.random.split(key_in, 4)
    hot_starts = jax.random.randint(sub_keys[0], (2,), 0, VOCAB_SIZE - HOT_WIDTH + 1)
    choice = jax.random.randint(sub_keys[1], (BATCH_ROWS,), 0, 4)
    offsets = jax.random.randint(sub_keys[2], (BATCH_ROWS,), 0, HOT_WIDTH)
    spread = jax.random.randint(sub_keys[3], (BATCH_ROWS,), 0, VOCAB_SIZE)
    hot_ids = jnp.where(choice == 3, hot_starts[1], hot_starts[0]) + offsets
    token_ids = jnp.where(choice == 0, spread, hot_ids)
    return token_ids.at[0].set(0).at[BATCH_ROWS - 1].set(VOCAB_SIZE - 1).astype(jnp.int32)


def setup_inputs(seed: int = 0, part: int = 0) -> dict:
    root_key = jax.random.key(seed)
    part_keys = jax.random.split(jax.random.fold_in(root_key, part), 2)
    weight_keys = jax.random.split(root_key, 10)
    hidden = (2.0 * jax.random.normal(part_keys[0], (BATCH_ROWS, MODEL_DIM), jnp.float32)).astype(jnp.bfloat16)
    tokens = draw_tokens(part_keys[1])
    embedding = jax.random.normal(weight_keys[0], (VOCAB_SIZE, MODEL_DIM), jnp.float32).astype(jnp.bfloat16)
    head_w = (jax.random.normal(weight_keys[1], (MODEL_DIM, VOCAB_SIZE), jnp.float32) * (1.5 * MODEL_DIM ** -0.5)).astype(jnp.bfloat16)
    h_norm = 1.0 + 0.5 * jax.random.normal(weight_keys[2], (MODEL_DIM,), jnp.float32)
    e_norm = 1.0 + 0.5 * jax.random.normal(weight_keys[3], (MODEL_DIM,), jnp.float32)
    f_norm = 1.0 + 0.5 * jax.random.normal(weight_keys[4], (MODEL_DIM,), jnp.float32)
    o_norm = 1.0 + 0.5 * jax.random.normal(weight_keys[5], (MODEL_DIM,), jnp.float32)
    proj_w = (jax.random.normal(weight_keys[6], (2 * MODEL_DIM, MODEL_DIM), jnp.float32) * (2 * MODEL_DIM) ** -0.5).astype(jnp.bfloat16)
    w_gate = (jax.random.normal(weight_keys[7], (MODEL_DIM, FFN_DIM), jnp.float32) * MODEL_DIM ** -0.5).astype(jnp.bfloat16)
    w_up = (jax.random.normal(weight_keys[8], (MODEL_DIM, FFN_DIM), jnp.float32) * MODEL_DIM ** -0.5).astype(jnp.bfloat16)
    w_down = (jax.random.normal(weight_keys[9], (FFN_DIM, MODEL_DIM), jnp.float32) * FFN_DIM ** -0.5).astype(jnp.bfloat16)
    return {"hidden": hidden, "tokens": tokens, "embedding": embedding, "head_w": head_w, "h_norm": h_norm, "e_norm": e_norm, "f_norm": f_norm, "o_norm": o_norm, "proj_w": proj_w, "w_gate": w_gate, "w_up": w_up, "w_down": w_down}


def rms_norm(values, norm_gain):
    wide_vals = values.astype(jnp.float32)
    inv_rms = lax.rsqrt(jnp.mean(wide_vals * wide_vals, axis=-1, keepdims=True) + NORM_EPS)
    return wide_vals * inv_rms * norm_gain


def reference(hidden, tokens, embedding, head_w, h_norm, e_norm, f_norm, o_norm, proj_w, w_gate, w_up, w_down):
    emb_rows = jnp.take(embedding, tokens, axis=0)
    joined = jnp.concatenate([rms_norm(hidden, h_norm), rms_norm(emb_rows, e_norm)], axis=-1).astype(jnp.bfloat16)
    proj_full = jnp.dot(joined, proj_w, preferred_element_type=jnp.float32).astype(jnp.bfloat16)
    normed = rms_norm(proj_full, f_norm).astype(jnp.bfloat16)
    gate_val = jnp.dot(normed, w_gate, preferred_element_type=jnp.float32)
    up_val = jnp.dot(normed, w_up, preferred_element_type=jnp.float32)
    act_val = (jax.nn.silu(gate_val) * up_val).astype(jnp.bfloat16)
    down_val = jnp.dot(act_val, w_down, preferred_element_type=jnp.float32)
    new_u = (proj_full.astype(jnp.float32) + down_val).astype(jnp.bfloat16)
    out_norm = rms_norm(new_u, o_norm).astype(jnp.bfloat16)
    logits = jnp.dot(out_norm, head_w, preferred_element_type=jnp.float32)
    log_total = jax.nn.logsumexp(logits, axis=-1, keepdims=True)
    return new_u, logits - log_total
```

```python
import functools

import jax
import jax.numpy as jnp
from jax import lax
from jax.experimental import pallas as pl
from jax.experimental.pallas import tpu as pltpu
from jax.sharding import PartitionSpec as P

NORM_EPS = 1e-6
MESH = pl.DeviceIdType.MESH
TP = 8
HEAD_TILE = 512
FINISH_TILE = 512


def rms_norm(values, norm_gain):
    wide_vals = values.astype(jnp.float32)
    inv_rms = lax.rsqrt(jnp.mean(wide_vals * wide_vals, axis=-1, keepdims=True) + NORM_EPS)
    return wide_vals * inv_rms * norm_gain


def head_kernel(vocab, tile, o_ref, w_ref, z_ref, stats_ref, m_ref, s_ref):
    step = pl.program_id(0)
    steps = pl.num_programs(0)
    rows = o_ref.shape[0]

    @pl.when(step == 0)
    def _():
        m_ref[...] = jnp.full(m_ref.shape, -jnp.inf, jnp.float32)
        s_ref[...] = jnp.zeros(s_ref.shape, jnp.float32)

    def account(z):
        groups = z.reshape(z.shape[0] // 8, 8, rows)
        m_old = m_ref[...]
        m_new = jnp.maximum(m_old, jnp.max(groups, axis=0))
        m_ref[...] = m_new
        s_ref[...] = s_ref[...] * jnp.exp(m_old - m_new) + jnp.sum(jnp.exp(groups - m_new[None]), axis=0)

    def part(size):
        z = lax.dot_general(w_ref[pl.ds(0, size), :], o_ref[...], (((1,), (1,)), ((), ())), preferred_element_type=jnp.float32)
        z_ref[pl.ds(pl.multiple_of(step * tile, tile), size), :] = z
        account(z)

    @pl.when(step < steps - 1)
    def _():
        part(tile)

    @pl.when(step == steps - 1)
    def _():
        part(vocab - (pl.cdiv(vocab, tile) - 1) * tile)
        m_old = m_ref[...]
        m_row = jnp.max(m_old, axis=0, keepdims=True)
        s_row = jnp.sum(s_ref[...] * jnp.exp(m_old - m_row), axis=0, keepdims=True)
        stats_ref[0:1, :] = m_row
        stats_ref[1:2, :] = s_row


def lse_kernel(stats_ref, lse_ref, all_ref, send_sem, recv_sem):
    me = lax.axis_index("tp")
    barrier = pltpu.get_barrier_semaphore()
    for hop in range(1, TP):
        pl.semaphore_signal(barrier, inc=1, device_id={"tp": lax.rem(me + hop, TP)}, device_id_type=MESH)
    pl.semaphore_wait(barrier, TP - 1)
    copies = []
    for hop in range(1, TP):
        copy = pltpu.make_async_remote_copy(
            src_ref=stats_ref, dst_ref=all_ref.at[hop], send_sem=send_sem.at[hop], recv_sem=recv_sem.at[hop],
            device_id={"tp": lax.rem(me + hop, TP)}, device_id_type=MESH)
        copy.start()
        copies.append(copy)
    m = stats_ref[0:1, :]
    for copy in copies:
        copy.wait()
    for hop in range(1, TP):
        m = jnp.maximum(m, all_ref[hop, 0:1, :])
    s = stats_ref[1:2, :] * jnp.exp(stats_ref[0:1, :] - m)
    for hop in range(1, TP):
        s = s + all_ref[hop, 1:2, :] * jnp.exp(all_ref[hop, 0:1, :] - m)
    lse_ref[...] = jnp.broadcast_to(m + jnp.log(s), lse_ref.shape)


def finish_kernel(z_ref, lse_ref, out_ref):
    vocab = z_ref.shape[0]
    tile = out_ref.shape[0]
    step = pl.program_id(0)
    last = pl.num_programs(0) - 1

    def part(size):
        start = pl.multiple_of(step * tile, tile)
        out_ref[pl.ds(0, size), :] = z_ref[pl.ds(start, size), :] - lse_ref[0:1, :]

    @pl.when(step < last)
    def _():
        part(tile)

    @pl.when(step == last)
    def _():
        part(vocab - (pl.cdiv(vocab, tile) - 1) * tile)


def head(out_norm, head_t):
    rows, depth = out_norm.shape
    vocab = head_t.shape[0]
    steps = pl.cdiv(vocab, HEAD_TILE)
    z, stats = pl.pallas_call(
        functools.partial(head_kernel, vocab, HEAD_TILE),
        grid=(steps,),
        out_shape=(pltpu.VMEM((vocab, rows), jnp.float32), jax.ShapeDtypeStruct((2, rows), jnp.float32)),
        in_specs=[pl.BlockSpec(memory_space=pltpu.VMEM), pl.BlockSpec((HEAD_TILE, depth), lambda i: (i, 0))],
        out_specs=(pl.BlockSpec(memory_space=pltpu.VMEM), pl.BlockSpec(memory_space=pltpu.VMEM)),
        scratch_shapes=[pltpu.VMEM((8, rows), jnp.float32)] * 2,
        compiler_params=pltpu.CompilerParams(vmem_limit_bytes=7 * 2**20, dimension_semantics=("arbitrary",)),
        name="head",
    )(out_norm, head_t)
    lse = pl.pallas_call(
        lse_kernel,
        out_shape=jax.ShapeDtypeStruct((8, rows), jnp.float32),
        in_specs=[pl.BlockSpec(memory_space=pltpu.VMEM)],
        out_specs=pl.BlockSpec(memory_space=pltpu.VMEM),
        scratch_shapes=[pltpu.VMEM((TP, 2, rows), jnp.float32), pltpu.SemaphoreType.DMA((TP,)), pltpu.SemaphoreType.DMA((TP,))],
        compiler_params=pltpu.CompilerParams(vmem_limit_bytes=2**20, collective_id=0, has_side_effects=True),
        name="lse",
    )(stats)
    tile = FINISH_TILE
    logp_t = pl.pallas_call(
        finish_kernel,
        grid=(pl.cdiv(vocab, tile),),
        out_shape=jax.ShapeDtypeStruct((vocab, rows), jnp.float32),
        in_specs=[pl.BlockSpec(memory_space=pltpu.VMEM)] * 2,
        out_specs=pl.BlockSpec((tile, rows), lambda i: (i, 0)),
        compiler_params=pltpu.CompilerParams(vmem_limit_bytes=5 * 2**20, dimension_semantics=("arbitrary",)),
        name="finish",
    )(pltpu.with_memory_space_constraint(z, pltpu.VMEM), lse)
    return logp_t.T


def solution(mesh):
    def draft_step(hidden, tokens, embedding, head_w, h_norm, e_norm, f_norm, o_norm, proj_w, w_gate, w_up, w_down):
        tp_index = lax.axis_index("tp")
        vocab_local = embedding.shape[0]
        local_ids = tokens - tp_index * vocab_local
        owned_mask = (local_ids >= 0) & (local_ids < vocab_local)
        picked = jnp.take(embedding, jnp.clip(local_ids, 0, vocab_local - 1), axis=0)
        picked = jnp.where(owned_mask[:, None], picked, jnp.zeros_like(picked))
        emb_rows = lax.psum(picked, "tp")
        joined = jnp.concatenate([rms_norm(hidden, h_norm), rms_norm(emb_rows, e_norm)], axis=-1).astype(jnp.bfloat16)
        proj_cols = jnp.dot(joined, proj_w, preferred_element_type=jnp.float32).astype(jnp.bfloat16)
        proj_full = lax.all_gather(proj_cols, "tp", axis=1, tiled=True)
        normed = rms_norm(proj_full, f_norm).astype(jnp.bfloat16)
        gate_val = jnp.dot(normed, w_gate, preferred_element_type=jnp.float32)
        up_val = jnp.dot(normed, w_up, preferred_element_type=jnp.float32)
        act_val = (jax.nn.silu(gate_val) * up_val).astype(jnp.bfloat16)
        down_part = jnp.dot(act_val, w_down, preferred_element_type=jnp.float32)
        down_sum = lax.psum(down_part, "tp")
        new_u = (proj_full.astype(jnp.float32) + down_sum).astype(jnp.bfloat16)
        out_norm = rms_norm(new_u, o_norm).astype(jnp.bfloat16)
        return new_u, head(out_norm, head_w.T)

    specs_in = (P("dp", None), P("dp"), P("tp", None), P(None, "tp"), P(None), P(None), P(None), P(None), P(None, "tp"), P(None, "tp"), P(None, "tp"), P("tp", None))
    specs_out = (P("dp", None), P("dp", "tp"))
    return jax.shard_map(draft_step, mesh=mesh, in_specs=specs_in, out_specs=specs_out, check_vma=False)
```

```python
import functools

import jax
import jax.numpy as jnp
from jax import lax
from jax.experimental import pallas as pl
from jax.experimental.pallas import tpu as pltpu
from jax.sharding import PartitionSpec as P

NORM_EPS = 1e-6
MESH = pl.DeviceIdType.MESH
TP = 8
HEAD_TILE = 512
FINISH_TILE = 512
BLOCKS = 3
STAGGER = 1
GROUP = 16
CHUNKS = 8
NT = (((1,), (1,)), ((), ()))
NN = (((1,), (0,)), ((), ()))
TN = (((0,), (0,)), ((), ()))
VMEM = pl.BlockSpec(memory_space=pltpu.VMEM)
ANY = pl.BlockSpec(memory_space=pl.ANY)
MIB = 2**20


def on_chip(shape, dtype):
    return pltpu.VMEM(shape, dtype)


def pinned(array):
    return pltpu.with_memory_space_constraint(array, pltpu.VMEM)


def dot(lhs, rhs, dims):
    return lax.dot_general(lhs, rhs, dims, preferred_element_type=jnp.float32)


def gather_kernel(vocab, tok_ref, emb_ref, out_ref, tiles_ref, sems):
    rows, depth = out_ref.shape
    per_chunk = rows // CHUNKS
    base = lax.axis_index("tp") * vocab

    def copy(i, chunk):
        local = jnp.clip(tok_ref[i] - base, 0, vocab - 1)
        start = pl.multiple_of(lax.shift_left(lax.shift_right_logical(local, 3), 3), 8)
        return pltpu.make_async_copy(emb_ref.at[pl.ds(start, 8), :], tiles_ref.at[i], sems.at[chunk])

    def issue(chunk, first, count):
        for j in range(count):
            copy(chunk * per_chunk + first + j, chunk).start()

    def issue_chunk(chunk):
        def body(g, carry):
            issue(chunk, g * GROUP, GROUP)
            return carry

        lax.fori_loop(0, per_chunk // GROUP, body, 0)

    issue_chunk(0)
    issue_chunk(1)
    row_id = lax.broadcasted_iota(jnp.int32, (8, depth), 0)

    def chunk_body(chunk, carry):
        pltpu.make_async_copy(
            tiles_ref.at[pl.ds(chunk * per_chunk, per_chunk)], tiles_ref.at[pl.ds(chunk * per_chunk, per_chunk)], sems.at[chunk]
        ).wait()

        @pl.when(chunk + 2 < CHUNKS)
        def _():
            issue_chunk(chunk + 2)

        def group_body(g, carry):
            first = pl.multiple_of(chunk * per_chunk + g * GROUP, GROUP)
            halves = []
            for half in range(GROUP // 8):
                acc = jnp.zeros((8, depth), jnp.float32)
                for j in range(8):
                    i = first + half * 8 + j
                    local = tok_ref[i] - base
                    owned = jnp.logical_and(local >= 0, local < vocab)
                    turn = jnp.bitwise_and(j + 8 - jnp.bitwise_and(local, 7), 7)
                    tile = pltpu.roll(tiles_ref[i].astype(jnp.float32), turn, 0)
                    acc = jnp.where(row_id == jnp.where(owned, j, -1), tile, acc)
                halves.append(acc)
            out_ref[pl.ds(first, GROUP), :] = jnp.concatenate(halves, axis=0).astype(jnp.bfloat16)
            return carry

        lax.fori_loop(0, per_chunk // GROUP, group_body, 0)
        return carry

    lax.fori_loop(0, CHUNKS, chunk_body, 0)


def gather_rows(tokens, embedding):
    rows = tokens.shape[0]
    vocab, depth = embedding.shape
    return pl.pallas_call(
        functools.partial(gather_kernel, vocab),
        out_shape=on_chip((rows, depth), jnp.bfloat16),
        in_specs=[pl.BlockSpec(memory_space=pltpu.SMEM), ANY],
        out_specs=VMEM,
        scratch_shapes=[pltpu.VMEM((rows, 8, depth), jnp.bfloat16), pltpu.SemaphoreType.DMA((CHUNKS,))],
        compiler_params=pltpu.CompilerParams(vmem_limit_bytes=24 * MIB),
        name="gather",
    )(tokens, embedding)


def front_kernel(
    part_ref, hidden_ref, hg_ref, eg_ref, fg_ref, og_ref, pw_hbm, wg_hbm, wu_hbm, wd_hbm,
    u_ref, ot_ref,
    pw_ref, wg_ref, wu_ref, wd_ref, hc_ref, ec_ref, ph_ref, n_ref, a_ref, down_ref,
    e_pair, e_sx, e_sy, e_rx, e_ry, e_tx, e_ty, e_qx, e_qy, e_keep, e_all,
    d_pair, d_sx, d_sy, d_rx, d_ry, d_tx, d_ty, d_qx, d_qy, d_keep,
    p_all, u_all, send_sems, recv_sems, load_sems,
):
    me = lax.axis_index("tp")
    core = lax.rem(me, 2)
    other = 1 - core
    chip = me // 2
    flip_x = 1 - 2 * lax.rem(chip, 2)
    flip_y = 2 - 4 * (me // 4)
    chip_x, chip_y, chip_d = chip + flip_x, chip + flip_y, 3 - chip
    dev_pair, dev_x, dev_y = me + 1 - 2 * core, me + 2 * flip_x, me + 2 * flip_y

    barrier = pltpu.get_barrier_semaphore()
    for device in (dev_pair, dev_x, dev_y):
        pl.semaphore_signal(barrier, inc=1, device_id={"tp": device}, device_id_type=MESH)

    loads = []
    for i, (src, dst) in enumerate(((pw_hbm, pw_ref), (wg_hbm, wg_ref), (wu_hbm, wu_ref), (wd_hbm, wd_ref))):
        load = pltpu.make_async_copy(src, dst, load_sems.at[i])
        load.start()
        loads.append(load)
    pl.semaphore_wait(barrier, 3)

    started = []

    def sender(b):
        count = [0]

        def send(src, dst, device):
            i = count[0]
            count[0] += 1
            copy = pltpu.make_async_remote_copy(
                src_ref=src, dst_ref=dst, send_sem=send_sems.at[b, i], recv_sem=recv_sems.at[b, i],
                device_id={"tp": device}, device_id_type=MESH)
            copy.start()
            started.append(copy)
            return copy

        return send

    block = hidden_ref.shape[0] // BLOCKS
    depth = hidden_ref.shape[1]

    def wide(x):
        return x.astype(jnp.float32)

    def reduce_scatter(b, send, mine, pair, sx, sy, rx, ry, tx, ty, qx, qy, keep, finish):
        dtype = sx.dtype
        first = send(mine.at[:, other], pair.at[b], dev_pair)
        yield
        first.wait_recv()

        def pair_sum(k, half):
            return wide(mine[k, core, half]) + wide(pair[b, k, half])

        sx[b, 0] = pair_sum(chip_x, 0).astype(dtype)
        sx[b, 1] = pair_sum(chip_d, 0).astype(dtype)
        copy_x = send(sx.at[b], rx.at[b], dev_x)
        sy[b, 0] = pair_sum(chip_y, 1).astype(dtype)
        sy[b, 1] = pair_sum(chip_d, 1).astype(dtype)
        copy_y = send(sy.at[b], ry.at[b], dev_y)
        yield
        copy_x.wait_recv()
        ty[b] = (pair_sum(chip_y, 0) + wide(rx[b, 1])).astype(dtype)
        pass_y = send(ty.at[b], qy.at[b], dev_y)
        copy_y.wait_recv()
        tx[b] = (pair_sum(chip_x, 1) + wide(ry[b, 1])).astype(dtype)
        pass_x = send(tx.at[b], qx.at[b], dev_x)
        keep[b, 0] = (pair_sum(chip, 0) + wide(rx[b, 0])).astype(dtype)
        keep[b, 1] = (pair_sum(chip, 1) + wide(ry[b, 0])).astype(dtype)
        yield
        pass_y.wait_recv()
        finish(0, wide(keep[b, 0]) + wide(qy[b]))
        pass_x.wait_recv()
        finish(1, wide(keep[b, 1]) + wide(qx[b]))

    def all_gather(b, send, full):
        own = full.at[chip, core]
        own_x = send(own, own, dev_x)
        own_y = send(own, own, dev_y)
        arrivals = [send(own, own, dev_pair)]
        yield
        own_x.wait_recv()
        from_x = full.at[chip_x, core]
        on_y = send(full.at[chip_x, core, 0], full.at[chip_x, core, 0], dev_y)
        arrivals.append(send(from_x, from_x, dev_pair))
        own_y.wait_recv()
        from_y = full.at[chip_y, core]
        on_x = send(full.at[chip_y, core, 1], full.at[chip_y, core, 1], dev_x)
        arrivals.append(send(from_y, from_y, dev_pair))
        yield
        on_y.wait_recv()
        diag0 = full.at[chip_d, core, 0]
        arrivals.append(send(diag0, diag0, dev_pair))
        on_x.wait_recv()
        diag1 = full.at[chip_d, core, 1]
        arrivals.append(send(diag1, diag1, dev_pair))
        yield
        for arrival in arrivals:
            arrival.wait_recv()

    def norm_rows(src, dst, gain_ref):
        def body(i, carry):
            rows = pl.ds(pl.multiple_of(i * 32, 32), 32)
            x = wide(src(rows))
            inv = lax.rsqrt(jnp.mean(x * x, axis=-1, keepdims=True) + NORM_EPS)
            dst[rows, :] = (x * inv * gain_ref[...]).astype(jnp.bfloat16)
            return carry

        return body

    def norm_columns(full, gain_ref, dst):
        n = full.shape[3]
        total = jnp.zeros((8, block), jnp.float32)
        for i in range(TP * 2):
            x = wide(full[i // 4, (i // 2) % 2, i % 2])
            total = total + jnp.sum((x * x).reshape(n // 8, 8, block), axis=0)
        inv = lax.rsqrt(jnp.sum(total, axis=0, keepdims=True) / depth + NORM_EPS)
        for i in range(TP * 2):
            x = wide(full[i // 4, (i // 2) % 2, i % 2])
            dst(i * n, n, (x * inv * gain_ref[i * n:(i + 1) * n, :]).astype(jnp.bfloat16))

    def run(b):
        send = sender(b)
        cols = pl.ds(b * block, block)
        rows_per_half = block // 16

        def e_finish(half, total):
            e_all[b, chip, core, half] = total.astype(jnp.bfloat16)

        gen = reduce_scatter(b, send, part_ref.at[b], e_pair, e_sx, e_sy, e_rx, e_ry, e_tx, e_ty, e_qx, e_qy, e_keep, e_finish)
        next(gen)
        if b == 0:
            loads[0].wait()
        lax.fori_loop(0, block // 32, norm_rows(lambda rows: hidden_ref[pl.ds(b * block + rows.start, 32), :], hc_ref.at[b], hg_ref), 0)
        ph_ref[b] = dot(pw_ref[:, :depth], hc_ref[b], NT)
        yield
        for _ in gen:
            yield
        for _ in all_gather(b, send, e_all.at[b]):
            yield
        for i in range(16):
            x = wide(e_all[b, i // 4, (i // 2) % 2, i % 2])
            inv = lax.rsqrt(jnp.mean(x * x, axis=-1, keepdims=True) + NORM_EPS)
            ec_ref[b, i * rows_per_half:(i + 1) * rows_per_half, :] = (x * inv * eg_ref[...]).astype(jnp.bfloat16)
        piece = (ph_ref[b] + dot(pw_ref[:, depth:], ec_ref[b], NT)).astype(jnp.bfloat16)
        half_rows = piece.shape[0] // 2
        p_all[b, chip, core, 0] = piece[:half_rows]
        p_all[b, chip, core, 1] = piece[half_rows:]
        for _ in all_gather(b, send, p_all.at[b]):
            yield

        def n_store(start, size, value):
            n_ref[b, start:start + size, :] = value

        norm_columns(p_all.at[b], fg_ref, n_store)
        if b == 0:
            loads[1].wait()
            loads[2].wait()
        ffn = wg_ref.shape[0]
        step = ffn // 2
        for i in range(2):
            span = slice(i * step, (i + 1) * step)
            gate = dot(wg_ref[span, :], n_ref[b], NN)
            up = dot(wu_ref[span, :], n_ref[b], NN)
            a_ref[b, span, :] = (jax.nn.silu(gate) * up).astype(jnp.bfloat16)
        if b == 0:
            loads[3].wait()
        pieces = 2
        width = depth // TP
        for i in range(TP // pieces):
            down = dot(wd_ref[:, i * pieces * width:(i + 1) * pieces * width], a_ref[b], TN)
            for j in range(pieces * 2):
                half = down[j * half_rows:(j + 1) * half_rows]
                d = i * pieces + j // 2
                down_ref[b, d // 2, d % 2, j % 2] = half

        def d_finish(half, total):
            u_all[b, chip, core, half] = (wide(p_all[b, chip, core, half]) + total).astype(jnp.bfloat16)

        yield from reduce_scatter(b, send, down_ref.at[b], d_pair, d_sx, d_sy, d_rx, d_ry, d_tx, d_ty, d_qx, d_qy, d_keep, d_finish)
        yield from all_gather(b, send, u_all.at[b])

        def o_store(start, size, value):
            ot_ref[start:start + size, b * block:(b + 1) * block] = value

        norm_columns(u_all.at[b], og_ref, o_store)
        for i in range(TP):
            piece = u_all[b, i // 2, i % 2].reshape(2 * half_rows, block)
            n_ref[b, i * 2 * half_rows:(i + 1) * 2 * half_rows, :] = piece
        u_ref[b * block:(b + 1) * block, :] = n_ref[b].T

    runs = [run(b) for b in range(BLOCKS)]
    live = set(range(BLOCKS))
    tick = 0
    while live:
        for b in range(BLOCKS):
            if b in live and tick >= b * STAGGER:
                try:
                    next(runs[b])
                except StopIteration:
                    live.discard(b)
        tick += 1
    for copy in started:
        copy.wait_send()


COPIES = 2 * 5 + 3 * 9


def front(part, hidden, h_norm, e_norm, f_norm, o_norm, proj_t, gate_t, up_t, w_down):
    rows, depth = hidden.shape
    block = rows // BLOCKS
    width = proj_t.shape[0]
    ffn = gate_t.shape[0]
    part = part.reshape(BLOCKS, 4, 2, 2, block // 16, depth)
    bf16, f32 = jnp.bfloat16, jnp.float32

    def exchange(dtype, n, m):
        shapes = [(4, 2, n, m)] + [(2, n, m)] * 4 + [(n, m)] * 4 + [(2, n, m)]
        return [pltpu.VMEM((BLOCKS, *shape), dtype) for shape in shapes]

    return pl.pallas_call(
        front_kernel,
        out_shape=(jax.ShapeDtypeStruct((rows, depth), bf16), on_chip((depth, rows), bf16)),
        in_specs=[VMEM] * 6 + [ANY] * 4,
        out_specs=(VMEM, VMEM),
        scratch_shapes=[
            pltpu.VMEM(proj_t.shape, bf16), pltpu.VMEM(gate_t.shape, bf16), pltpu.VMEM(up_t.shape, bf16), pltpu.VMEM(w_down.shape, bf16),
            pltpu.VMEM((BLOCKS, block, depth), bf16), pltpu.VMEM((BLOCKS, block, depth), bf16),
            pltpu.VMEM((BLOCKS, width, block), f32), pltpu.VMEM((BLOCKS, depth, block), bf16), pltpu.VMEM((BLOCKS, ffn, block), bf16),
            pltpu.VMEM((BLOCKS, 4, 2, 2, width // 2, block), f32),
            *exchange(bf16, block // 16, depth), pltpu.VMEM((BLOCKS, 4, 2, 2, block // 16, depth), bf16),
            *exchange(f32, width // 2, block),
            pltpu.VMEM((BLOCKS, 4, 2, 2, width // 2, block), bf16), pltpu.VMEM((BLOCKS, 4, 2, 2, width // 2, block), bf16),
            pltpu.SemaphoreType.DMA((BLOCKS, COPIES)), pltpu.SemaphoreType.DMA((BLOCKS, COPIES)), pltpu.SemaphoreType.DMA((4,)),
        ],
        compiler_params=pltpu.CompilerParams(vmem_limit_bytes=56 * MIB, collective_id=1, has_side_effects=True),
        name="front",
    )(pinned(part), hidden, h_norm.reshape(1, depth), e_norm.reshape(1, depth), f_norm.reshape(depth, 1), o_norm.reshape(depth, 1),
      proj_t, gate_t, up_t, w_down)


def head_kernel(vocab, tile, o_ref, w_ref, z_ref, stats_ref, m_ref, s_ref):
    step = pl.program_id(0)
    steps = pl.num_programs(0)
    rows = o_ref.shape[1]

    @pl.when(step == 0)
    def _():
        m_ref[...] = jnp.full(m_ref.shape, -jnp.inf, jnp.float32)
        s_ref[...] = jnp.zeros(s_ref.shape, jnp.float32)

    def account(z):
        groups = z.reshape(z.shape[0] // 8, 8, rows)
        m_old = m_ref[...]
        m_new = jnp.maximum(m_old, jnp.max(groups, axis=0))
        m_ref[...] = m_new
        s_ref[...] = s_ref[...] * jnp.exp(m_old - m_new) + jnp.sum(jnp.exp(groups - m_new[None]), axis=0)

    def part(size):
        z = dot(w_ref[pl.ds(0, size), :], o_ref[...], NN)
        z_ref[pl.ds(pl.multiple_of(step * tile, tile), size), :] = z
        account(z)

    @pl.when(step < steps - 1)
    def _():
        part(tile)

    @pl.when(step == steps - 1)
    def _():
        part(vocab - (pl.cdiv(vocab, tile) - 1) * tile)
        m_old = m_ref[...]
        m_row = jnp.max(m_old, axis=0, keepdims=True)
        s_row = jnp.sum(s_ref[...] * jnp.exp(m_old - m_row), axis=0, keepdims=True)
        stats_ref[0:1, :] = m_row
        stats_ref[1:2, :] = s_row


def lse_kernel(stats_ref, lse_ref, all_ref, send_sem, recv_sem):
    me = lax.axis_index("tp")
    barrier = pltpu.get_barrier_semaphore()
    for hop in range(1, TP):
        pl.semaphore_signal(barrier, inc=1, device_id={"tp": lax.rem(me + hop, TP)}, device_id_type=MESH)
    pl.semaphore_wait(barrier, TP - 1)
    copies = []
    for hop in range(1, TP):
        copy = pltpu.make_async_remote_copy(
            src_ref=stats_ref, dst_ref=all_ref.at[hop], send_sem=send_sem.at[hop], recv_sem=recv_sem.at[hop],
            device_id={"tp": lax.rem(me + hop, TP)}, device_id_type=MESH)
        copy.start()
        copies.append(copy)
    m = stats_ref[0:1, :]
    for copy in copies:
        copy.wait()
    for hop in range(1, TP):
        m = jnp.maximum(m, all_ref[hop, 0:1, :])
    s = stats_ref[1:2, :] * jnp.exp(stats_ref[0:1, :] - m)
    for hop in range(1, TP):
        s = s + all_ref[hop, 1:2, :] * jnp.exp(all_ref[hop, 0:1, :] - m)
    lse_ref[...] = jnp.broadcast_to(m + jnp.log(s), lse_ref.shape)


def finish_kernel(z_ref, lse_ref, out_ref):
    vocab = z_ref.shape[0]
    tile = out_ref.shape[0]
    step = pl.program_id(0)
    last = pl.num_programs(0) - 1

    def part(size):
        start = pl.multiple_of(step * tile, tile)
        out_ref[pl.ds(0, size), :] = z_ref[pl.ds(start, size), :] - lse_ref[0:1, :]

    @pl.when(step < last)
    def _():
        part(tile)

    @pl.when(step == last)
    def _():
        part(vocab - (pl.cdiv(vocab, tile) - 1) * tile)


def head(out_norm_t, head_t):
    depth, rows = out_norm_t.shape
    vocab = head_t.shape[0]
    z, stats = pl.pallas_call(
        functools.partial(head_kernel, vocab, HEAD_TILE),
        grid=(pl.cdiv(vocab, HEAD_TILE),),
        out_shape=(on_chip((vocab, rows), jnp.float32), jax.ShapeDtypeStruct((2, rows), jnp.float32)),
        in_specs=[VMEM, pl.BlockSpec((HEAD_TILE, depth), lambda i: (i, 0))],
        out_specs=(VMEM, VMEM),
        scratch_shapes=[pltpu.VMEM((8, rows), jnp.float32)] * 2,
        compiler_params=pltpu.CompilerParams(vmem_limit_bytes=5 * MIB, dimension_semantics=("arbitrary",)),
        name="head",
    )(pinned(out_norm_t), head_t)
    lse = pl.pallas_call(
        lse_kernel,
        out_shape=jax.ShapeDtypeStruct((8, rows), jnp.float32),
        in_specs=[VMEM],
        out_specs=VMEM,
        scratch_shapes=[pltpu.VMEM((TP, 2, rows), jnp.float32), pltpu.SemaphoreType.DMA((TP,)), pltpu.SemaphoreType.DMA((TP,))],
        compiler_params=pltpu.CompilerParams(vmem_limit_bytes=MIB, collective_id=0, has_side_effects=True),
        name="lse",
    )(stats)
    logp_t = pl.pallas_call(
        finish_kernel,
        grid=(pl.cdiv(vocab, FINISH_TILE),),
        out_shape=jax.ShapeDtypeStruct((vocab, rows), jnp.float32),
        in_specs=[VMEM, VMEM],
        out_specs=pl.BlockSpec((FINISH_TILE, rows), lambda i: (i, 0)),
        compiler_params=pltpu.CompilerParams(vmem_limit_bytes=5 * MIB, dimension_semantics=("arbitrary",)),
        name="finish",
    )(pinned(z), lse)
    return logp_t.T


def solution(mesh):
    def draft_step(hidden, tokens, embedding, head_w, h_norm, e_norm, f_norm, o_norm, proj_w, w_gate, w_up, w_down):
        part = gather_rows(tokens, embedding)
        new_u, out_norm_t = front(part, hidden, h_norm, e_norm, f_norm, o_norm, proj_w.T, w_gate.T, w_up.T, w_down)
        return new_u, head(out_norm_t, head_w.T)

    specs_in = (P("dp", None), P("dp"), P("tp", None), P(None, "tp"), P(None), P(None), P(None), P(None), P(None, "tp"), P(None, "tp"), P(None, "tp"), P("tp", None))
    specs_out = (P("dp", None), P("dp", "tp"))
    return jax.shard_map(draft_step, mesh=mesh, in_specs=specs_in, out_specs=specs_out, check_vma=False)
```

```python
import functools

import jax
import jax.numpy as jnp
from jax import lax
from jax.experimental import pallas as pl
from jax.experimental.pallas import tpu as pltpu
from jax.sharding import PartitionSpec as P

NORM_EPS = 1e-6
MESH = pl.DeviceIdType.MESH
TP = 8
HEAD_TILE = 480
FINISH_TILE = 144
SLOTS = 6
BLOCKS = 3
STAGGER = 1
GROUP = 16
CHUNKS = 8
NT = (((1,), (1,)), ((), ()))
NN = (((1,), (0,)), ((), ()))
TN = (((0,), (0,)), ((), ()))
VMEM = pl.BlockSpec(memory_space=pltpu.VMEM)
ANY = pl.BlockSpec(memory_space=pl.ANY)
MIB = 2**20
LOW = 3848 * 2**10
HIGH = 60840 * 2**10


def on_chip(shape, dtype):
    return pltpu.VMEM(shape, dtype)


def pinned(array):
    return pltpu.with_memory_space_constraint(array, pltpu.VMEM)


def dot(lhs, rhs, dims):
    return lax.dot_general(lhs, rhs, dims, preferred_element_type=jnp.float32)


def gather_kernel(vocab, tok_ref, emb_ref, out_ref, tiles_ref, sems):
    rows, depth = out_ref.shape
    per_chunk = rows // CHUNKS
    base = lax.axis_index("tp") * vocab

    def copy(i, chunk):
        local = tok_ref[i] - base
        owned = jnp.logical_and(local >= 0, local < vocab)
        start = pl.multiple_of(lax.shift_left(jnp.where(owned, lax.shift_right_logical(local, 3), i), 3), 8)
        return pltpu.make_async_copy(emb_ref.at[pl.ds(start, 8), :], tiles_ref.at[i], sems.at[chunk])

    def issue(chunk, first, count):
        for j in range(count):
            copy(chunk * per_chunk + first + j, chunk).start()

    def issue_chunk(chunk):
        def body(g, carry):
            issue(chunk, g * GROUP, GROUP)
            return carry

        lax.fori_loop(0, per_chunk // GROUP, body, 0)

    issue_chunk(0)
    issue_chunk(1)
    row_id = lax.broadcasted_iota(jnp.int32, (8, depth), 0)

    def chunk_body(chunk, carry):
        pltpu.make_async_copy(
            tiles_ref.at[pl.ds(chunk * per_chunk, per_chunk)], tiles_ref.at[pl.ds(chunk * per_chunk, per_chunk)], sems.at[chunk]
        ).wait()

        @pl.when(chunk + 2 < CHUNKS)
        def _():
            issue_chunk(chunk + 2)

        def group_body(g, carry):
            first = pl.multiple_of(chunk * per_chunk + g * GROUP, GROUP)
            halves = []
            for half in range(GROUP // 8):
                acc = jnp.zeros((8, depth), jnp.float32)
                for j in range(8):
                    i = first + half * 8 + j
                    local = tok_ref[i] - base
                    owned = jnp.logical_and(local >= 0, local < vocab)
                    turn = jnp.bitwise_and(j + 8 - jnp.bitwise_and(local, 7), 7)
                    tile = pltpu.roll(tiles_ref[i].astype(jnp.float32), turn, 0)
                    acc = jnp.where(row_id == jnp.where(owned, j, -1), tile, acc)
                halves.append(acc)
            out_ref[pl.ds(first, GROUP), :] = jnp.concatenate(halves, axis=0).astype(jnp.bfloat16)
            return carry

        lax.fori_loop(0, per_chunk // GROUP, group_body, 0)
        return carry

    lax.fori_loop(0, CHUNKS, chunk_body, 0)


def gather_rows(tokens, embedding):
    rows = tokens.shape[0]
    vocab, depth = embedding.shape
    return pl.pallas_call(
        functools.partial(gather_kernel, vocab),
        out_shape=on_chip((rows, depth), jnp.bfloat16),
        in_specs=[pl.BlockSpec(memory_space=pltpu.SMEM), ANY],
        out_specs=VMEM,
        scratch_shapes=[pltpu.VMEM((rows, 8, depth), jnp.bfloat16), pltpu.SemaphoreType.DMA((CHUNKS,))],
        compiler_params=pltpu.CompilerParams(vmem_limit_bytes=24 * MIB),
        name="gather",
    )(tokens, embedding)


def front_kernel(
    part_ref, hidden_ref, hg_ref, eg_ref, fg_ref, og_ref, pw_hbm, wg_hbm, wu_hbm, wd_hbm,
    u_ref, ot_ref,
    pw_ref, wg_ref, wu_ref, wd_ref, hc_ref, ec_ref, ph_ref, n_ref, a_ref, down_ref,
    e_pair, e_sx, e_sy, e_rx, e_ry, e_tx, e_ty, e_qx, e_qy, e_keep, e_all,
    d_pair, d_sx, d_sy, d_rx, d_ry, d_tx, d_ty, d_qx, d_qy, d_keep,
    p_all, u_all, fc_ref, oc_ref, send_sems, recv_sems, load_sems,
):
    me = lax.axis_index("tp")
    core = lax.rem(me, 2)
    other = 1 - core
    chip = me // 2
    flip_x = 1 - 2 * lax.rem(chip, 2)
    flip_y = 2 - 4 * (me // 4)
    chip_x, chip_y, chip_d = chip + flip_x, chip + flip_y, 3 - chip
    dev_pair, dev_x, dev_y = me + 1 - 2 * core, me + 2 * flip_x, me + 2 * flip_y

    barrier = pltpu.get_barrier_semaphore()
    for device in (dev_pair, dev_x, dev_y):
        pl.semaphore_signal(barrier, inc=1, device_id={"tp": device}, device_id_type=MESH)

    loads = []
    for i, (src, dst) in enumerate(((pw_hbm, pw_ref), (wg_hbm, wg_ref), (wu_hbm, wu_ref), (wd_hbm, wd_ref))):
        load = pltpu.make_async_copy(src, dst, load_sems.at[i])
        load.start()
        loads.append(load)
    pl.semaphore_wait(barrier, 3)

    started = []

    def sender(b):
        count = [0]

        def send(src, dst, device):
            i = count[0]
            count[0] += 1
            copy = pltpu.make_async_remote_copy(
                src_ref=src, dst_ref=dst, send_sem=send_sems.at[b, i], recv_sem=recv_sems.at[b, i],
                device_id={"tp": device}, device_id_type=MESH)
            copy.start()
            started.append(copy)
            return copy

        return send

    block = hidden_ref.shape[0] // BLOCKS
    depth = hidden_ref.shape[1]

    def wide(x):
        return x.astype(jnp.float32)

    def reduce_scatter(b, send, mine, pair, sx, sy, rx, ry, tx, ty, qx, qy, keep, finish):
        dtype = sx.dtype
        first = send(mine.at[:, other], pair.at[b], dev_pair)
        yield
        first.wait_recv()

        def pair_sum(k, half):
            return wide(mine[k, core, half]) + wide(pair[b, k, half])

        sx[b, 0] = pair_sum(chip_x, 0).astype(dtype)
        sx[b, 1] = pair_sum(chip_d, 0).astype(dtype)
        copy_x = send(sx.at[b], rx.at[b], dev_x)
        sy[b, 0] = pair_sum(chip_y, 1).astype(dtype)
        sy[b, 1] = pair_sum(chip_d, 1).astype(dtype)
        copy_y = send(sy.at[b], ry.at[b], dev_y)
        yield
        copy_x.wait_recv()
        ty[b] = (pair_sum(chip_y, 0) + wide(rx[b, 1])).astype(dtype)
        pass_y = send(ty.at[b], qy.at[b], dev_y)
        copy_y.wait_recv()
        tx[b] = (pair_sum(chip_x, 1) + wide(ry[b, 1])).astype(dtype)
        pass_x = send(tx.at[b], qx.at[b], dev_x)
        keep[b, 0] = (pair_sum(chip, 0) + wide(rx[b, 0])).astype(dtype)
        keep[b, 1] = (pair_sum(chip, 1) + wide(ry[b, 0])).astype(dtype)
        yield
        pass_y.wait_recv()
        finish(0, wide(keep[b, 0]) + wide(qy[b]))
        pass_x.wait_recv()
        finish(1, wide(keep[b, 1]) + wide(qx[b]))

    def all_gather(b, send, full):
        own = full.at[chip, core]
        own_x = send(own, own, dev_x)
        own_y = send(own, own, dev_y)
        arrivals = [send(own, own, dev_pair)]
        yield
        own_x.wait_recv()
        from_x = full.at[chip_x, core]
        on_y = send(full.at[chip_x, core, 0], full.at[chip_x, core, 0], dev_y)
        arrivals.append(send(from_x, from_x, dev_pair))
        own_y.wait_recv()
        from_y = full.at[chip_y, core]
        on_x = send(full.at[chip_y, core, 1], full.at[chip_y, core, 1], dev_x)
        arrivals.append(send(from_y, from_y, dev_pair))
        yield
        on_y.wait_recv()
        diag0 = full.at[chip_d, core, 0]
        arrivals.append(send(diag0, diag0, dev_pair))
        on_x.wait_recv()
        diag1 = full.at[chip_d, core, 1]
        arrivals.append(send(diag1, diag1, dev_pair))
        yield
        for arrival in arrivals:
            arrival.wait_recv()

    def norm_rows(src, dst, gain_ref):
        gain = gain_ref[...].reshape(1, depth)

        def body(i, carry):
            rows = pl.ds(pl.multiple_of(i * 32, 32), 32)
            x = wide(src(rows))
            inv = lax.rsqrt(jnp.mean(x * x, axis=-1, keepdims=True) + NORM_EPS)
            dst[rows, :] = (x * inv * gain).astype(jnp.bfloat16)
            return carry

        return body

    def norm_columns(full, gain_ref, dst):
        n = full.shape[3]
        total = jnp.zeros((8, block), jnp.float32)
        for i in range(TP * 2):
            x = wide(full[i // 4, (i // 2) % 2, i % 2])
            total = total + jnp.sum((x * x).reshape(n // 8, 8, block), axis=0)
        inv = lax.rsqrt(jnp.sum(total, axis=0, keepdims=True) / depth + NORM_EPS)
        for i in range(TP * 2):
            x = wide(full[i // 4, (i // 2) % 2, i % 2])
            gain = gain_ref[i * n:(i + 1) * n, :]
            dst(i * n, n, (x * inv * jnp.concatenate([gain] * (block // 128), axis=1)).astype(jnp.bfloat16))

    def run(b):
        send = sender(b)
        cols = pl.ds(b * block, block)
        rows_per_half = block // 16

        def e_finish(half, total):
            e_all[b, chip, core, half] = total.astype(jnp.bfloat16)

        gen = reduce_scatter(b, send, part_ref.at[b], e_pair, e_sx, e_sy, e_rx, e_ry, e_tx, e_ty, e_qx, e_qy, e_keep, e_finish)
        next(gen)
        if b == 0:
            for row_ref, column_ref in ((fg_ref, fc_ref), (og_ref, oc_ref)):
                for i in range(depth // 128):
                    lanes = row_ref[i * 128:(i + 1) * 128].reshape(1, 128)
                    column_ref[i * 128:(i + 1) * 128, :] = jnp.broadcast_to(lanes, (128, 128)).T
            loads[0].wait()
        lax.fori_loop(0, block // 32, norm_rows(lambda rows: hidden_ref[pl.ds(b * block + rows.start, 32), :], hc_ref.at[b], hg_ref), 0)
        ph_ref[b] = dot(pw_ref[:, :depth], hc_ref[b], NT)
        yield
        for _ in gen:
            yield
        for _ in all_gather(b, send, e_all.at[b]):
            yield
        for i in range(16):
            x = wide(e_all[b, i // 4, (i // 2) % 2, i % 2])
            inv = lax.rsqrt(jnp.mean(x * x, axis=-1, keepdims=True) + NORM_EPS)
            ec_ref[b, i * rows_per_half:(i + 1) * rows_per_half, :] = (x * inv * eg_ref[...].reshape(1, depth)).astype(jnp.bfloat16)
        piece = (ph_ref[b] + dot(pw_ref[:, depth:], ec_ref[b], NT)).astype(jnp.bfloat16)
        half_rows = piece.shape[0] // 2
        p_all[b, chip, core, 0] = piece[:half_rows]
        p_all[b, chip, core, 1] = piece[half_rows:]
        for _ in all_gather(b, send, p_all.at[b]):
            yield

        def n_store(start, size, value):
            n_ref[b, start:start + size, :] = value

        norm_columns(p_all.at[b], fc_ref, n_store)
        if b == 0:
            loads[1].wait()
            loads[2].wait()
        ffn = wg_ref.shape[0]
        step = ffn // 2
        for i in range(2):
            span = slice(i * step, (i + 1) * step)
            gate = dot(wg_ref[span, :], n_ref[b], NN)
            up = dot(wu_ref[span, :], n_ref[b], NN)
            a_ref[b, span, :] = (jax.nn.silu(gate) * up).astype(jnp.bfloat16)
        if b == 0:
            loads[3].wait()
        pieces = 2
        width = depth // TP
        for i in range(TP // pieces):
            down = dot(wd_ref[:, i * pieces * width:(i + 1) * pieces * width], a_ref[b], TN)
            for j in range(pieces * 2):
                half = down[j * half_rows:(j + 1) * half_rows]
                d = i * pieces + j // 2
                down_ref[b, d // 2, d % 2, j % 2] = half

        def d_finish(half, total):
            u_all[b, chip, core, half] = (wide(p_all[b, chip, core, half]) + total).astype(jnp.bfloat16)

        yield from reduce_scatter(b, send, down_ref.at[b], d_pair, d_sx, d_sy, d_rx, d_ry, d_tx, d_ty, d_qx, d_qy, d_keep, d_finish)
        yield from all_gather(b, send, u_all.at[b])

        def o_store(start, size, value):
            ot_ref[start:start + size, b * block:(b + 1) * block] = value

        norm_columns(u_all.at[b], oc_ref, o_store)
        for i in range(TP):
            piece = u_all[b, i // 2, i % 2].reshape(2 * half_rows, block)
            n_ref[b, i * 2 * half_rows:(i + 1) * 2 * half_rows, :] = piece
        u_ref[b * block:(b + 1) * block, :] = n_ref[b].T

    runs = [run(b) for b in range(BLOCKS)]
    live = set(range(BLOCKS))
    tick = 0
    while live:
        for b in range(BLOCKS):
            if b in live and tick >= b * STAGGER:
                try:
                    next(runs[b])
                except StopIteration:
                    live.discard(b)
        tick += 1
    for copy in started:
        copy.wait_send()


COPIES = 2 * 5 + 3 * 9


def front(part, hidden, h_norm, e_norm, f_norm, o_norm, proj_t, gate_t, up_t, w_down):
    rows, depth = hidden.shape
    block = rows // BLOCKS
    width = proj_t.shape[0]
    ffn = gate_t.shape[0]
    part = part.reshape(BLOCKS, 4, 2, 2, block // 16, depth)
    bf16, f32 = jnp.bfloat16, jnp.float32

    def exchange(dtype, n, m):
        shapes = [(4, 2, n, m)] + [(2, n, m)] * 4 + [(n, m)] * 4 + [(2, n, m)]
        return [pltpu.VMEM((BLOCKS, *shape), dtype) for shape in shapes]

    return pl.pallas_call(
        front_kernel,
        out_shape=(jax.ShapeDtypeStruct((rows, depth), bf16), on_chip((depth, rows), bf16)),
        in_specs=[VMEM] * 6 + [ANY] * 4,
        out_specs=(VMEM, VMEM),
        scratch_shapes=[
            pltpu.VMEM(proj_t.shape, bf16), pltpu.VMEM(gate_t.shape, bf16), pltpu.VMEM(up_t.shape, bf16), pltpu.VMEM(w_down.shape, bf16),
            pltpu.VMEM((BLOCKS, block, depth), bf16), pltpu.VMEM((BLOCKS, block, depth), bf16),
            pltpu.VMEM((BLOCKS, width, block), f32), pltpu.VMEM((BLOCKS, depth, block), bf16), pltpu.VMEM((BLOCKS, ffn, block), bf16),
            pltpu.VMEM((BLOCKS, 4, 2, 2, width // 2, block), f32),
            *exchange(bf16, block // 16, depth), pltpu.VMEM((BLOCKS, 4, 2, 2, block // 16, depth), bf16),
            *exchange(f32, width // 2, block),
            pltpu.VMEM((BLOCKS, 4, 2, 2, width // 2, block), bf16), pltpu.VMEM((BLOCKS, 4, 2, 2, width // 2, block), bf16),
            pltpu.VMEM((depth, 128), f32), pltpu.VMEM((depth, 128), f32),
            pltpu.SemaphoreType.DMA((BLOCKS, COPIES)), pltpu.SemaphoreType.DMA((BLOCKS, COPIES)), pltpu.SemaphoreType.DMA((4,)),
        ],
        compiler_params=pltpu.CompilerParams(vmem_limit_bytes=HIGH, collective_id=1, has_side_effects=True),
        name="front",
    )(pinned(part), hidden, h_norm, e_norm, f_norm, o_norm,
      proj_t, gate_t, up_t, w_down)


def head_kernel(tile, o_ref, w_hbm, z_ref, stats_ref, w_ref, m_ref, s_ref, sems):
    vocab = w_hbm.shape[0]
    rows = o_ref.shape[1]
    full = vocab // tile
    tail = vocab - full * tile

    def load(step, slot, size):
        start = pl.multiple_of(step * tile, tile)
        return pltpu.make_async_copy(w_hbm.at[pl.ds(start, size), :], w_ref.at[slot, pl.ds(0, size), :], sems.at[slot])

    def part(step, slot, size):
        load(step, slot, size).wait()
        z = dot(w_ref[slot, :size, :], o_ref[...], NN)
        z_ref[pl.ds(pl.multiple_of(step * tile, tile), size), :] = z
        groups = z.reshape(size // 8, 8, rows)
        m_old = m_ref[...]
        m_new = jnp.maximum(m_old, jnp.max(groups, axis=0))
        m_ref[...] = m_new
        s_ref[...] = s_ref[...] * jnp.exp(m_old - m_new) + jnp.sum(jnp.exp(groups - m_new[None]), axis=0)

    load(0, 0, tile).start()
    load(1, 1, tile).start()
    m_ref[...] = jnp.full(m_ref.shape, -jnp.inf, jnp.float32)
    s_ref[...] = jnp.zeros(s_ref.shape, jnp.float32)

    def body(i, carry):
        for slot in range(2):
            part(2 * i + slot, slot, tile)
            load(2 * i + slot + 2, slot, tile).start()
        return carry

    pairs = (full - 2) // 2
    lax.fori_loop(0, pairs, body, 0)
    for step in range(2 * pairs, full):
        part(step, step % 2, tile)
        after = step + 2
        if after < full:
            load(after, step % 2, tile).start()
        elif after == full:
            load(after, step % 2, tail).start()
    part(full, full % 2, tail)
    m_old = m_ref[...]
    m_row = jnp.max(m_old, axis=0, keepdims=True)
    s_row = jnp.sum(s_ref[...] * jnp.exp(m_old - m_row), axis=0, keepdims=True)
    stats_ref[0:1, :] = m_row
    stats_ref[1:2, :] = s_row


def lse_kernel(stats_ref, lse_ref, all_ref, send_sem, recv_sem):
    me = lax.axis_index("tp")
    barrier = pltpu.get_barrier_semaphore()
    for hop in range(1, TP):
        pl.semaphore_signal(barrier, inc=1, device_id={"tp": lax.rem(me + hop, TP)}, device_id_type=MESH)
    pl.semaphore_wait(barrier, TP - 1)
    copies = []
    for hop in range(1, TP):
        copy = pltpu.make_async_remote_copy(
            src_ref=stats_ref, dst_ref=all_ref.at[hop], send_sem=send_sem.at[hop], recv_sem=recv_sem.at[hop],
            device_id={"tp": lax.rem(me + hop, TP)}, device_id_type=MESH)
        copy.start()
        copies.append(copy)
    m = stats_ref[0:1, :]
    for copy in copies:
        copy.wait()
    for hop in range(1, TP):
        m = jnp.maximum(m, all_ref[hop, 0:1, :])
    s = stats_ref[1:2, :] * jnp.exp(stats_ref[0:1, :] - m)
    for hop in range(1, TP):
        s = s + all_ref[hop, 1:2, :] * jnp.exp(all_ref[hop, 0:1, :] - m)
    lse_ref[...] = jnp.broadcast_to(m + jnp.log(s), lse_ref.shape)


def finish_kernel(tile, z_ref, lse_ref, out_ref, ring_ref, sems):
    vocab = z_ref.shape[0]
    steps = pl.cdiv(vocab, tile)
    tail = vocab - (steps - 1) * tile
    lse = lse_ref[0:1, :]

    def copy(step, slot, size):
        start = pl.multiple_of(step * tile, tile)
        return pltpu.make_async_copy(ring_ref.at[slot, pl.ds(0, size), :], out_ref.at[pl.ds(start, size), :], sems.at[slot])

    def put(step, size):
        slot = lax.rem(step, SLOTS)
        start = pl.multiple_of(step * tile, tile)
        ring_ref[slot, pl.ds(0, size), :] = z_ref[pl.ds(start, size), :] - lse
        copy(step, slot, size).start()

    for step in range(SLOTS):
        put(step, tile)

    def body(step, carry):
        copy(step - SLOTS, lax.rem(step, SLOTS), tile).wait()
        put(step, tile)
        return carry

    lax.fori_loop(SLOTS, steps - 1, body, 0)
    last = steps - 1
    copy(last - SLOTS, last % SLOTS, tile).wait()
    put(last, tail)
    for step in range(steps - SLOTS, steps):
        copy(step, step % SLOTS, tail if step == last else tile).wait()


def head(out_norm_t, head_t):
    depth, rows = out_norm_t.shape
    vocab = head_t.shape[0]
    z, stats = pl.pallas_call(
        functools.partial(head_kernel, HEAD_TILE),
        out_shape=(on_chip((vocab, rows), jnp.float32), jax.ShapeDtypeStruct((2, rows), jnp.float32)),
        in_specs=[VMEM, ANY],
        out_specs=(VMEM, VMEM),
        scratch_shapes=[pltpu.VMEM((2, HEAD_TILE, depth), jnp.bfloat16)] + [pltpu.VMEM((8, rows), jnp.float32)] * 2 + [pltpu.SemaphoreType.DMA((2,))],
        compiler_params=pltpu.CompilerParams(vmem_limit_bytes=LOW),
        name="head",
    )(pinned(out_norm_t), head_t)
    lse = pl.pallas_call(
        lse_kernel,
        out_shape=jax.ShapeDtypeStruct((8, rows), jnp.float32),
        in_specs=[VMEM],
        out_specs=VMEM,
        scratch_shapes=[pltpu.VMEM((TP, 2, rows), jnp.float32), pltpu.SemaphoreType.DMA((TP,)), pltpu.SemaphoreType.DMA((TP,))],
        compiler_params=pltpu.CompilerParams(vmem_limit_bytes=MIB, collective_id=0, has_side_effects=True),
        name="lse",
    )(stats)
    logp_t = pl.pallas_call(
        functools.partial(finish_kernel, FINISH_TILE),
        out_shape=jax.ShapeDtypeStruct((vocab, rows), jnp.float32),
        in_specs=[VMEM, VMEM],
        out_specs=ANY,
        scratch_shapes=[pltpu.VMEM((SLOTS, FINISH_TILE, rows), jnp.float32), pltpu.SemaphoreType.DMA((SLOTS,))],
        compiler_params=pltpu.CompilerParams(vmem_limit_bytes=LOW),
        name="finish",
    )(pinned(z), lse)
    return logp_t.T


def solution(mesh):
    def draft_step(hidden, tokens, embedding, head_w, h_norm, e_norm, f_norm, o_norm, proj_w, w_gate, w_up, w_down):
        part = gather_rows(tokens, embedding)
        new_u, out_norm_t = front(part, hidden, h_norm, e_norm, f_norm, o_norm, proj_w.T, w_gate.T, w_up.T, w_down)
        return new_u, head(out_norm_t, head_w.T)

    specs_in = (P("dp", None), P("dp"), P("tp", None), P(None, "tp"), P(None), P(None), P(None), P(None), P(None, "tp"), P(None, "tp"), P(None, "tp"), P("tp", None))
    specs_out = (P("dp", None), P("dp", "tp"))
    return jax.shard_map(draft_step, mesh=mesh, in_specs=specs_in, out_specs=specs_out, check_vma=False)
```
